32 devices in a mesh: grp: 2 (over x), gx: 8 (over z, y), gy: 2 (over core).
Axes of the slice: x: 2, y: 2, z: 4, core: 2. Of those that a mesh axis runs over, the one named last changes fastest.
Arguments:
- flow_state: float32 [2, 4, 128, 16, 128], P('grp', None, 'gx', 'gy'), may hold values from -6 to 6
- block_offset: int32 [32], P('gx'), may hold values from -3 to 3, as said below
- block_weight: float32 [32], P('gx'), may hold values from 0.1 to 0.9
Outputs:
- advanced: float32 [2, 4, 128, 16, 128], P('grp', None, 'gx', 'gy')
The draws below stay inside these ranges and needn't reach their ends.
Inputs may be any that keep to these rules, and one draw needn't show every extreme that they name: Block b's lamb reaches blocks b + block_offset[b] and the next one, counted modulo 32; in every brick of 4 blocks the first block has a negative offset and the last block an offset of 0 or more.
All inputs are finite; a program needn't handle non-finite values.
Results may differ from the reference program's by a relative error of at most 0.00005.
Values sent between devices are 32-bit elements; how exact they have to be, the bound alone decides.
No kernel may reach another device: no remote copies, remote signals or barrier semaphores. Data moves between devices by JAX's collectives and lax.ppermute only.
A program may use at most 64 MiB of HBM per device.

```python
import jax
import jax.numpy as jnp
from jax import lax

NZ = 128
NB = 4
NX = 128
NY = 16
NBT = 32


def draw_flow_state(key, part):
    return jax.random.truncated_normal(key, -6.0, 6.0, (2, 4, NX, NY, NZ), jnp.float32)


def draw_block_offset(key, part):
    middle = jax.random.randint(jax.random.fold_in(key, 101), (NBT,), 1 - NB, NB, dtype=jnp.int32)
    leading = jax.random.randint(jax.random.fold_in(key, 202), (NBT,), 1 - NB, 0, dtype=jnp.int32)
    trailing = jax.random.randint(jax.random.fold_in(key, 303), (NBT,), 0, NB, dtype=jnp.int32)
    within = jnp.arange(NBT, dtype=jnp.int32) % NB
    chosen = jnp.where(within == 0, leading, middle)
    return jnp.where(within == NB - 1, trailing, chosen).astype(jnp.int32)


def level_of(key, dims, shards, smallest, largest):
    factor_of = 1.0
    for dim, parts in shards:
        draws = jax.random.uniform(jax.random.fold_in(jax.random.fold_in(key, 6), dim), (parts,), jnp.float32, smallest / len(shards), largest / len(shards))
        factor_of = factor_of * jnp.repeat(jnp.exp(draws), dims[dim] // parts).reshape((-1,) + (1,) * (len(dims) - 1 - dim))
    return factor_of


def setup_inputs(seed: int = 0) -> dict:
    arg_keys = jax.random.split(jax.random.key(seed), 4)
    flow_state = draw_flow_state(jax.random.fold_in(arg_keys[3], 71), 0)
    block_offset = draw_block_offset(jax.random.fold_in(arg_keys[3], 71), 0)
    block_weight = jnp.clip(0.1 + 0.79999997 * jax.random.uniform(arg_keys[2], (NBT,), jnp.float32) ** level_of(arg_keys[2], (NBT,), ((0, 8),), -0.2, 0.2), 0.1, 0.9)
    return dict(flow_state=flow_state, block_offset=block_offset, block_weight=block_weight)


drp_weights = (0.907646591371, -0.337048393268, 0.133442885327, -0.045246480208, 0.011169294114, -0.001456501759)
viscosity = 0.05
mean_flow = 0.5
les_time_step = 0.1
ape_time_step = 0.4


def shifted(extended, margin, direction, offset_j):
    width_x = extended.shape[1] - 2 * margin
    width_y = extended.shape[2] - 2 * margin
    if direction == 1:
        return extended[:, margin + offset_j:margin + offset_j + width_x, margin:margin + width_y]
    if direction == 2:
        return extended[:, margin:margin + width_x, margin + offset_j:margin + offset_j + width_y]
    centre = extended[:, margin:margin + width_x, margin:margin + width_y]
    return jnp.roll(centre, -offset_j, axis=3)


def derivative(extended, margin, weight_list, direction):
    total = None
    for offset_j, weight_j in enumerate(weight_list, start=1):
        term = weight_j * (shifted(extended, margin, direction, offset_j) - shifted(extended, margin, direction, -offset_j))
        total = term if total is None else total + term
    return total


def les_tendency(extended, margin):
    grad_x, grad_y, grad_z = [derivative(extended, margin, (0.5,), direction) for direction in (1, 2, 3)]
    centre = shifted(extended, margin, 1, 0)
    vel_x, vel_y, vel_z = centre[0], centre[1], centre[2]
    vort_x = grad_y[2] - grad_z[1]
    vort_y = grad_z[0] - grad_x[2]
    vort_z = grad_x[1] - grad_y[0]
    lamb_vec = jnp.stack([vort_y * vel_z - vort_z * vel_y, vort_z * vel_x - vort_x * vel_z, vort_x * vel_y - vort_y * vel_x])
    spread = -6.0 * centre
    for direction in (1, 2, 3):
        spread = spread + shifted(extended, margin, direction, 1) + shifted(extended, margin, direction, -1)
    tend_vel = -lamb_vec + viscosity * spread[:3]
    tend_scalar = -(vel_x * grad_x[3] + vel_y * grad_y[3] + vel_z * grad_z[3]) + viscosity * spread[3]
    return jnp.concatenate([tend_vel, tend_scalar[None]], axis=0), lamb_vec


def ape_tendency(extended, margin, source):
    grad_x, grad_y, grad_z = [derivative(extended, margin, drp_weights, direction) for direction in (1, 2, 3)]
    tend_press = -mean_flow * grad_x[0] - (grad_x[1] + grad_y[2] + grad_z[3])
    tend_vel = -mean_flow * grad_x[1:] - jnp.stack([grad_x[0], grad_y[0], grad_z[0]]) - source
    return jnp.concatenate([tend_press[None], tend_vel], axis=0)


def extend(whole, margin):
    padded = jnp.pad(whole, ((0, 0), (margin, margin), (0, 0), (0, 0)), mode="wrap")
    return jnp.pad(padded, ((0, 0), (0, 0), (margin, margin), (0, 0)))


def deposit(lamb_vec, block_offset, block_weight):
    block_count = block_offset.shape[0]
    blocks = lamb_vec.reshape(3, block_count, -1)
    anchor = jnp.arange(block_count, dtype=jnp.int32)
    target = (anchor + block_offset) % block_count
    following = (target + 1) % block_count
    columns = jnp.arange(block_count, dtype=jnp.int32)
    matrix = jnp.where(columns[None, :] == target[:, None], block_weight[:, None], 0.0)
    matrix = matrix + jnp.where(columns[None, :] == following[:, None], 1.0 - block_weight[:, None], 0.0)
    moved = jnp.einsum("bs,cbk->csk", matrix, blocks, precision=lax.Precision.HIGHEST)
    return moved.reshape(lamb_vec.shape)


def tendencies(fields, block_offset, block_weight):
    les_part, lamb_vec = les_tendency(extend(fields[0], 1), 1)
    source = deposit(lamb_vec, block_offset, block_weight)
    ape_part = ape_tendency(extend(fields[1], 6), 6, source)
    return jnp.stack([les_part, ape_part])


def reference(flow_state, block_offset, block_weight):
    steps_both = jnp.array([les_time_step, ape_time_step], dtype=flow_state.dtype)[:, None, None, None, None]
    predicted = flow_state + steps_both * tendencies(flow_state, block_offset, block_weight)
    corrected = predicted + steps_both * tendencies(predicted, block_offset, block_weight)
    return 0.5 * (flow_state + corrected)
```

```python
import jax
import jax.numpy as jnp
from jax import lax
from jax.experimental import pallas as pl
from jax.experimental.pallas import tpu as pltpu
from jax.sharding import PartitionSpec as P

drp_weights = (
    0.907646591371,
    -0.337048393268,
    0.133442885327,
    -0.045246480208,
    0.011169294114,
    -0.001456501759,
)
viscosity = 0.05
mean_flow = 0.5
les_time_step = 0.1
ape_time_step = 0.4
reach = len(drp_weights)


class Plan:
    def __init__(self, cells, blocks, rows, gy_size):
        self.n, self.nb, self.rows = cells, blocks, rows
        self.bc = cells // blocks
        self.gy = gy_size
        n, nb, bc = self.n, self.nb, self.bc
        self.t_lo = (-reach) // bc
        self.t_hi = (n + reach - 1) // bc
        span = range(-3 * nb, 4 * nb)
        self.src = {t: [b for b in span if t in self.reached(b)] for t in range(self.t_lo, self.t_hi + 1)}
        self.b1 = sorted({b for t in self.src for b in self.src[t]})
        self.b2 = sorted({b for t in range(nb) for b in self.src[t]})
        self.l2_lo, self.l2_hi = self.b2[0] * bc, (self.b2[-1] + 1) * bc
        self.pr_lo, self.pr_hi = self.l2_lo - 1, self.l2_hi + 1
        self.extra = [b for b in self.b1 if b not in self.b2]
        need = set(range(self.pr_lo - 1, self.pr_hi + 1))
        for b in self.extra:
            need |= set(range(b * bc - 1, (b + 1) * bc + 1))
        self.f_lo, self.f_hi = min(need), max(need) + 1
        self.les = {k: [c - k * n for c in sorted(need) if k * n <= c < (k + 1) * n] for k in (-2, -1, 1, 2)}
        assert not [c for c in need if not -2 * n <= c < 3 * n]
        self.wide = 2 * reach
        assert self.wide <= n and self.l2_hi <= 2 * n and self.l2_lo >= -n
        self.ape = {-1: list(range(n - self.wide, n)), 1: list(range(self.wide))}
        self.size = {}
        for k in (-2, -1, 1, 2):
            tiles = 3 * len(self.les[k]) + (2 if abs(k) == 1 else 0) + 1
            if abs(k) == 1:
                tiles = max(tiles, 4 * self.wide)
            self.size[k] = tiles
        self.depth = -(-self.wide // rows)
        if gy_size == 1:
            self.steps, self.slots = [], 1
        elif gy_size == 2:
            self.steps, self.slots = [None], 2
        else:
            self.steps = [d for d in range(-self.depth, self.depth + 1) if d]
            self.slots = 2 * self.depth + 1
        self.height = (self.slots + 2) * rows

    def reached(self, block):
        within = block % self.nb
        low = 1 - self.nb if within < self.nb - 1 else 0
        high = self.nb - 1 if within > 0 else -1
        return range(block + low, block + high + 2)

    def own_slot(self):
        if self.gy == 1:
            return 0
        return lax.axis_index("gy") if self.gy == 2 else self.depth

    def slot_of(self, step):
        return 1 - lax.axis_index("gy") if step is None else self.depth + step

    def near(self):
        return [s for s in self.steps if s is None or abs(s) == 1]

    def inside(self, step):
        if step is None:
            return None
        row = lax.axis_index("gy") + step
        return jnp.where((row >= 0) & (row < self.gy), 1.0, 0.0).astype(jnp.float32)

    def row(self, slot):
        return self.rows + self.rows * slot


def runs(values):
    out = []
    for pos, v in enumerate(values):
        if out and out[-1][0] + out[-1][2] == v:
            out[-1][2] += 1
        else:
            out.append([v, pos, 1])
    return out


def roll_z(tile, j):
    width = tile.shape[-1]
    return pltpu.roll(tile, (-j) % width, tile.ndim - 1)


def pack_kernel(plan, off_ref, wgt_ref, x_ref, *outs):
    n, nb = plan.n, plan.nb
    out_of = dict(zip((-2, -1, 1, 2), outs))
    is_les = lax.axis_index("grp") == 0

    @pl.when(is_les)
    def _():
        rowid = lax.broadcasted_iota(jnp.int32, x_ref.shape[-2:], 0)
        info = jnp.zeros(x_ref.shape[-2:], jnp.float32)
        for k in range(nb):
            info = jnp.where(rowid == k, off_ref[k].astype(jnp.float32), info)
            info = jnp.where(rowid == nb + k, wgt_ref[k], info)
        for k, out in out_of.items():
            cells = plan.les[k]
            for c in range(3):
                for first, pos, length in runs(cells):
                    at = c * len(cells) + pos
                    out[at : at + length] = x_ref[0, c, first : first + length]
            at = 3 * len(cells)
            if abs(k) == 1:
                first = n - 2 if k < 0 else 0
                out[at : at + 2] = x_ref[0, 3, first : first + 2]
                at += 2
            out[at] = info

    @pl.when(jnp.logical_not(is_les))
    def _():
        for k, out in out_of.items():
            if abs(k) == 1:
                first = plan.ape[k][0]
                for c in range(4):
                    out[c * plan.wide : (c + 1) * plan.wide] = x_ref[0, c, first : first + plan.wide]
            else:
                out[...] = jnp.zeros_like(out)


def load(ref, c, cell, row, rows=8):
    return ref[c, cell, pl.ds(row, rows), :]


def les_point(ref, cell, row, comps, spread_of):
    own = [load(ref, c, cell, row) for c in range(comps)]
    xp = [load(ref, c, cell + 1, row) for c in range(comps)]
    xm = [load(ref, c, cell - 1, row) for c in range(comps)]
    yp = [load(ref, c, cell, row + 1) for c in range(comps)]
    ym = [load(ref, c, cell, row - 1) for c in range(comps)]
    zp = [roll_z(f, 1) for f in own]
    zm = [roll_z(f, -1) for f in own]
    vort_x = (yp[2] - ym[2]) - (zp[1] - zm[1])
    vort_y = (zp[0] - zm[0]) - (xp[2] - xm[2])
    vort_z = (xp[1] - xm[1]) - (yp[0] - ym[0])
    lamb = [
        0.5 * (vort_y * own[2] - vort_z * own[1]),
        0.5 * (vort_z * own[0] - vort_x * own[2]),
        0.5 * (vort_x * own[1] - vort_y * own[0]),
    ]
    spread = [
        ((xp[c] + xm[c]) + (yp[c] + ym[c])) + (zp[c] + zm[c]) - 6.0 * own[c] for c in spread_of
    ]
    tend = [viscosity * s for s in spread]
    if comps == 4 and len(tend) == 4:
        moved = (
            own[0] * (xp[3] - xm[3]) + own[1] * (yp[3] - ym[3]) + own[2] * (zp[3] - zm[3])
        )
        tend[3] = tend[3] - 0.5 * moved
    for c in range(min(3, len(tend))):
        tend[c] = tend[c] - lamb[c]
    return own, lamb, tend


def gather_les(plan, dst, comps, x, near, messages, base, cells_lo, cells_hi):
    row = base
    for c in range(comps):
        dst[c, -cells_lo : plan.n - cells_lo, pl.ds(row, plan.rows), :] = x[c]
        for k, ref in messages.items():
            cells = plan.les[k]
            if c < 3:
                for first, pos, length in runs(cells):
                    lo = max(first + k * plan.n, cells_lo)
                    hi = min(first + length + k * plan.n, cells_hi)
                    if lo >= hi:
                        continue
                    at = c * len(cells) + pos + lo - (first + k * plan.n)
                    dst[c, lo - cells_lo : hi - cells_lo, pl.ds(row, plan.rows), :] = ref[at : at + hi - lo]
            elif abs(k) == 1:
                at = 3 * len(cells)
                lo = -2 if k < 0 else plan.n
                dst[c, lo - cells_lo : lo + 2 - cells_lo, pl.ds(row, plan.rows), :] = ref[at : at + 2]


def source_kernel(plan, off_ref, wgt_ref, *refs):
    msgs = 5
    tiles = [refs[i * msgs : (i + 1) * msgs] for i in range(1 + len(plan.steps))]
    out_ref = refs[msgs * len(tiles)]
    field, pred, lamb1, lamb2, side, summed, summed_y, ape, ape_d = refs[msgs * len(tiles) + 1 :]
    is_les = lax.axis_index("grp") == 0
    keys = (-2, -1, 1, 2)

    @pl.when(is_les)
    def _():
        les_source(plan, off_ref, wgt_ref, tiles, keys, out_ref, field, pred, lamb1, lamb2, side, summed, summed_y)

    @pl.when(jnp.logical_not(is_les))
    def _():
        ape_base(plan, tiles, keys, out_ref, ape, ape_d)


def pads(plan):
    return (0, (plan.slots + 1) * plan.rows)


def open_pad(plan):
    if plan.gy == 2:
        return [plan.own_slot() * (plan.slots + 1) * plan.rows]
    return list(pads(plan)) if plan.slots == 1 else []


def les_source(plan, off_ref, wgt_ref, tiles, keys, out_ref, field, pred, lamb1, lamb2, side, summed, summed_y):
    n, nb, bc, rows = plan.n, plan.nb, plan.bc, plan.rows
    own = plan.row(plan.own_slot())
    zero_cells = jnp.zeros((field.shape[1], rows, field.shape[3]), jnp.float32)
    for c in range(3):
        for pad in pads(plan):
            field[c, :, pl.ds(pad, rows), :] = zero_cells
        for pad in open_pad(plan):
            pred[c, :, pl.ds(pad, rows), :] = zero_cells[: pred.shape[1]]
    gather_les(plan, field, 3, tiles[0][0][0], False, dict(zip(keys, tiles[0][1:])), own, plan.f_lo, plan.f_hi)
    for step, tile in zip(plan.steps, tiles[1:]):
        gather_les(plan, field, 3, tile[0][0], True, dict(zip(keys, tile[1:])), plan.row(plan.slot_of(step)), plan.f_lo, plan.f_hi)

    def first(i, carry):
        cell = i + plan.pr_lo - plan.f_lo
        here, lamb, tend = les_point(field, cell, own, 3, (0, 1, 2))
        for c in range(3):
            lamb1[c, cell] = lamb[c]
            pred[c, i, pl.ds(own, rows), :] = here[c] + les_time_step * tend[c]
        for k, step in enumerate(plan.near()):
            row = plan.row(plan.slot_of(step))
            inside = plan.inside(step)
            here, lamb, tend = les_point(field, cell, row, 3, (0, 1, 2))
            moved = [here[c] + les_time_step * tend[c] for c in range(3)]
            if inside is not None:
                lamb[1] = lamb[1] * inside
                moved = [m * inside for m in moved]
            side[k, cell] = lamb[1]
            for c in range(3):
                pred[c, i, pl.ds(row, rows), :] = moved[c]
        return carry

    lax.fori_loop(0, plan.pr_hi - plan.pr_lo, first, 0)

    for lo, _, length in runs([b * bc + k - plan.f_lo for b in plan.extra for k in range(bc)]):

        def more(i, carry, lo=lo):
            _, lamb, _ = les_point(field, lo + i, own, 3, ())
            for c in range(3):
                lamb1[c, lo + i] = lamb[c]
            return carry

        lax.fori_loop(0, length, more, 0, unroll=2)

    def second(i, carry):
        _, lamb, _ = les_point(pred, i + plan.l2_lo - plan.pr_lo, own, 3, ())
        for c in range(3):
            lamb2[c, i + plan.l2_lo - plan.f_lo] = lamb[c]
        return carry

    lax.fori_loop(0, plan.l2_hi - plan.l2_lo, second, 0, unroll=2)

    shape = (rows, field.shape[3])
    info = {k: ref for k, ref in zip(keys, tiles[0][1:])}

    def maps(b):
        k = b // nb
        i = b % nb
        if k == 0:
            return (
                jnp.full(shape, off_ref[i].astype(jnp.float32), jnp.float32),
                jnp.full(shape, wgt_ref[i], jnp.float32),
            )
        at = 3 * len(plan.les[k]) + (2 if abs(k) == 1 else 0)
        return (
            jnp.broadcast_to(info[k][at, i : i + 1, :], shape),
            jnp.broadcast_to(info[k][at, nb + i : nb + i + 1, :], shape),
        )

    near = plan.near()
    pad_tile = jnp.zeros((n, rows, field.shape[3]), jnp.float32)
    for pad in open_pad(plan):
        summed_y[:, pl.ds(pad, rows), :] = pad_tile
    for t in range(plan.t_lo, plan.t_hi + 1):
        shares = []
        for b in plan.src[t]:
            off, wgt = maps(b)
            shares.append((b, jnp.where(off == t - b, wgt, jnp.where(off == t - b - 1, 1.0 - wgt, 0.0))))
        first_cell = max(t * bc, -reach)
        last_cell = min((t + 1) * bc, n + reach)
        inner = 0 <= t < nb

        def total(ref, c, k):
            acc = None
            for b, share in shares:
                term = share * ref[c, b * bc - plan.f_lo + k]
                acc = term if acc is None else acc + term
            return acc

        def step_k(k, carry, t=t, inner=inner, total=total):
            for c in range(3):
                s1 = total(lamb1, c, k)
                summed[c, t * bc + k + reach] = s1
                if inner:
                    out_ref[0, c + 1, t * bc + k] = s1 + total(lamb2, c, k)
                    if c == 1:
                        summed_y[t * bc + k, pl.ds(own, rows), :] = s1
            if inner:
                for q, step in enumerate(near):
                    summed_y[t * bc + k, pl.ds(plan.row(plan.slot_of(step)), rows), :] = total(side, q, k)
            return carry

        lax.fori_loop(first_cell - t * bc, last_cell - t * bc, step_k, 0)

    half_two = 0.5 * ape_time_step * ape_time_step

    def finish(i, carry):
        grads = []
        for c in range(3):
            acc = None
            for j, wt in enumerate(drp_weights, start=1):
                term = wt * (summed[c, i + reach + j] - summed[c, i + reach - j])
                acc = term if acc is None else acc + term
            grads.append(acc)
        div = grads[0]
        for j, wt in enumerate(drp_weights, start=1):
            div = div + wt * (summed_y[i, pl.ds(own + j, rows), :] - summed_y[i, pl.ds(own - j, rows), :])
        mid = summed[2, i + reach]
        for j, wt in enumerate(drp_weights, start=1):
            div = div + wt * (roll_z(mid, j) - roll_z(mid, -j))
        out_ref[0, 0, i] = half_two * div
        for c in range(3):
            out_ref[0, c + 1, i] = (half_two * mean_flow) * grads[c] - (0.5 * ape_time_step) * out_ref[0, c + 1, i]
        return carry

    lax.fori_loop(0, n, finish, 0)


def ape_point(ref, cell, row, comps):
    def along_x(c):
        acc = None
        for j, wt in enumerate(drp_weights, start=1):
            term = wt * (load(ref, c, cell + j, row) - load(ref, c, cell - j, row))
            acc = term if acc is None else acc + term
        return acc

    def along_y(c):
        acc = None
        for j, wt in enumerate(drp_weights, start=1):
            term = wt * (load(ref, c, cell, row + j) - load(ref, c, cell, row - j))
            acc = term if acc is None else acc + term
        return acc

    def along_z(c):
        mid = load(ref, c, cell, row)
        acc = None
        for j, wt in enumerate(drp_weights, start=1):
            term = wt * (roll_z(mid, j) - roll_z(mid, -j))
            acc = term if acc is None else acc + term
        return acc

    xs = {0: along_x(0), 1: along_x(1)}
    out = {0: -mean_flow * xs[0] - (xs[1] + along_y(2) + along_z(3))}
    if 1 in comps:
        out[1] = -mean_flow * xs[1] - xs[0]
    if 2 in comps:
        out[2] = -mean_flow * along_x(2) - along_y(0)
    if 3 in comps:
        out[3] = -mean_flow * along_x(3) - along_z(0)
    return out


def ape_base(plan, tiles, keys, out_ref, ape, ape_d):
    n, rows, wide = plan.n, plan.rows, plan.wide
    own = plan.row(plan.own_slot())
    blank = jnp.zeros((ape.shape[1], rows, ape.shape[3]), jnp.float32)
    for c in (0, 2):
        for pad in pads(plan):
            ape[c, wide : wide + n, pl.ds(pad, rows), :] = blank[:n]
        for pad in open_pad(plan):
            ape_d[c, reach : reach + n, pl.ds(pad, rows), :] = blank[:n]
    for c in (0, 2):
        for pad in open_pad(plan):
            ape[c, reach:wide, pl.ds(pad, rows), :] = blank[: wide - reach]
            ape[c, wide + n : wide + n + reach, pl.ds(pad, rows), :] = blank[:reach]
    for step, tile in zip([0] + plan.steps, tiles):
        main = tile is tiles[0]
        row = own if main else plan.row(plan.slot_of(step))
        msg = dict(zip(keys, tile[1:]))
        cut = wide if main else reach
        for c in range(4):
            ape[c, wide : wide + n, pl.ds(row, rows), :] = tile[0][0, c]
            left, right = msg[-1], msg[1]
            ape[c, wide - cut : wide, pl.ds(row, rows), :] = left[(c + 1) * wide - cut : (c + 1) * wide]
            ape[c, wide + n : wide + n + cut, pl.ds(row, rows), :] = right[c * wide : c * wide + cut]

    def first(i, carry):
        got = ape_point(ape, i + reach, own, (0, 1, 2, 3))
        for c in range(4):
            ape_d[c, i, pl.ds(own, rows), :] = got[c]
        return carry

    lax.fori_loop(0, n + 2 * reach, first, 0)

    for step in plan.near():
        row = plan.row(plan.slot_of(step))
        inside = plan.inside(step)

        def beside(i, carry, row=row, inside=inside):
            got = ape_point(ape, i + wide, row, (0, 2))
            for c in (0, 2):
                ape_d[c, i + reach, pl.ds(row, rows), :] = got[c] if inside is None else got[c] * inside
            return carry

        lax.fori_loop(0, n, beside, 0)

    half_two = 0.5 * ape_time_step * ape_time_step

    def second(i, carry):
        got = ape_point(ape_d, i + reach, own, (0, 1, 2, 3))
        for c in range(4):
            here = load(ape, c, i + wide, own)
            rate = load(ape_d, c, i + reach, own)
            out_ref[0, c, i] = here + ape_time_step * rate + half_two * got[c]
        return carry

    lax.fori_loop(0, n, second, 0)


def les_kernel(plan, *refs):
    msgs = 3
    tiles = [refs[i * msgs : (i + 1) * msgs] for i in range(1 + len(plan.steps))]
    out_ref, field, pred = refs[msgs * len(tiles) :]

    @pl.when(lax.axis_index("grp") == 0)
    def _():
        n, rows = plan.n, plan.rows
        own = plan.row(plan.own_slot())
        blank = jnp.zeros((n + 4, rows, field.shape[3]), jnp.float32)
        for c in range(4):
            for pad in pads(plan):
                field[c, :, pl.ds(pad, rows), :] = blank
            for pad in open_pad(plan):
                pred[c, :, pl.ds(pad, rows), :] = blank[: n + 2]
        gather_les(plan, field, 4, tiles[0][0][0], False, dict(zip((-1, 1), tiles[0][1:])), own, -2, n + 2)
        for step, tile in zip(plan.steps, tiles[1:]):
            gather_les(plan, field, 4, tile[0][0], True, dict(zip((-1, 1), tile[1:])), plan.row(plan.slot_of(step)), -2, n + 2)

        def first(i, carry):
            here, _, tend = les_point(field, i + 1, own, 4, (0, 1, 2, 3))
            for c in range(4):
                pred[c, i, pl.ds(own, rows), :] = here[c] + les_time_step * tend[c]
            for step in plan.near():
                row = plan.row(plan.slot_of(step))
                inside = plan.inside(step)
                here, _, tend = les_point(field, i + 1, row, 4, (0, 1, 2, 3))
                for c in range(4):
                    moved = here[c] + les_time_step * tend[c]
                    pred[c, i, pl.ds(row, rows), :] = moved if inside is None else moved * inside
            return carry

        lax.fori_loop(0, n + 2, first, 0)

        def second(i, carry):
            here, _, tend = les_point(pred, i + 1, own, 4, (0, 1, 2, 3))
            for c in range(4):
                start = load(field, c, i + 2, own)
                out_ref[0, c, i] = 0.5 * (start + (here[c] + les_time_step * tend[c]))
            return carry

        lax.fori_loop(0, n, second, 0)


def smem():
    return pl.BlockSpec(memory_space=pltpu.SMEM)


def vmem():
    return pl.BlockSpec(memory_space=pltpu.VMEM)


def on_device(flow_state, block_offset, block_weight):
    comps, n, rows, nz = flow_state.shape[1:]
    groups, ring, walls = [lax.axis_size(a) for a in ("grp", "gx", "gy")]
    plan = Plan(n, block_offset.shape[0], rows, walls)
    f32 = jnp.float32
    keys = (-2, -1, 1, 2)
    packed = pl.pallas_call(
        lambda *r: pack_kernel(plan, *r),
        name="pack",
        in_specs=[smem(), smem(), vmem()],
        out_specs=[vmem()] * 4,
        out_shape=[jax.ShapeDtypeStruct((plan.size[k], rows, nz), f32) for k in keys],
    )(block_offset, block_weight, flow_state)

    def along(block, shift):
        return lax.ppermute(block, "gx", [((i + shift) % ring, i) for i in range(ring)])

    def beside(block, step):
        if step is None:
            return lax.ppermute(block, "gy", [(0, 1), (1, 0)])
        return lax.ppermute(block, "gy", [(i + step, i) for i in range(walls) if 0 <= i + step < walls])

    got = [along(p, k) for k, p in zip(keys, packed)]
    tiles = [[flow_state] + got]
    for step in plan.steps:
        tiles.append([beside(flow_state, step)] + [beside(g, step) for g in got])

    def scratch(*shape):
        return pltpu.VMEM(shape, f32)

    cells = plan.f_hi - plan.f_lo
    h = plan.height
    part = pl.pallas_call(
        lambda *r: source_kernel(plan, *r),
        name="source",
        in_specs=[smem(), smem()] + [vmem()] * (5 * len(tiles)),
        out_specs=vmem(),
        out_shape=jax.ShapeDtypeStruct(flow_state.shape, f32),
        scratch_shapes=[
            scratch(3, cells, h, nz),
            scratch(3, plan.pr_hi - plan.pr_lo, h, nz),
            scratch(3, cells, rows, nz),
            scratch(3, cells, rows, nz),
            scratch(max(1, len(plan.near())), cells, rows, nz),
            scratch(3, n + 2 * reach, rows, nz),
            scratch(n, h, nz),
            scratch(4, n + 2 * plan.wide, h, nz),
            scratch(4, n + 2 * reach, h, nz),
        ],
    )(block_offset, block_weight, *[a for t in tiles for a in t])
    handed = lax.ppermute(part, "grp", [(i, (i + 1) % groups) for i in range(groups)])
    les = pl.pallas_call(
        lambda *r: les_kernel(plan, *r),
        name="les",
        in_specs=[vmem()] * (3 * len(tiles)),
        out_specs=vmem(),
        out_shape=jax.ShapeDtypeStruct(flow_state.shape, f32),
        scratch_shapes=[scratch(4, n + 4, h, nz), scratch(4, n + 2, h, nz)],
    )(*[a for t in tiles for a in (t[0], t[2], t[3])])
    return jnp.where(lax.axis_index("grp") == 0, les, part + handed)


def solution(mesh):
    placed = (P("grp", None, "gx", "gy", None), P("gx"), P("gx"))
    return jax.shard_map(
        on_device,
        mesh=mesh,
        in_specs=placed,
        out_specs=P("grp", None, "gx", "gy", None),
        check_vma=False,
    )
```

```python
import jax
import jax.numpy as jnp
from jax import lax
from jax.experimental import pallas as pl
from jax.experimental.pallas import tpu as pltpu
from jax.sharding import PartitionSpec as P

drp_weights = (
    0.907646591371,
    -0.337048393268,
    0.133442885327,
    -0.045246480208,
    0.011169294114,
    -0.001456501759,
)
viscosity = 0.05
mean_flow = 0.5
les_time_step = 0.1
ape_time_step = 0.4
reach = len(drp_weights)


class Plan:
    def __init__(self, cells, blocks, rows, gy_size):
        self.n, self.nb, self.rows = cells, blocks, rows
        self.bc = cells // blocks
        self.gy = gy_size
        n, nb, bc = self.n, self.nb, self.bc
        self.t_lo = (-reach) // bc
        self.t_hi = (n + reach - 1) // bc
        span = range(-3 * nb, 4 * nb)
        self.src = {t: [b for b in span if t in self.reached(b)] for t in range(self.t_lo, self.t_hi + 1)}
        self.b1 = sorted({b for t in self.src for b in self.src[t]})
        self.b2 = sorted({b for t in range(nb) for b in self.src[t]})
        self.l2_lo, self.l2_hi = self.b2[0] * bc, (self.b2[-1] + 1) * bc
        self.pr_lo, self.pr_hi = self.l2_lo - 1, self.l2_hi + 1
        self.extra = [b for b in self.b1 if b not in self.b2]
        need = set(range(self.pr_lo - 1, self.pr_hi + 1))
        for b in self.extra:
            need |= set(range(b * bc - 1, (b + 1) * bc + 1))
        self.f_lo, self.f_hi = min(need), max(need) + 1
        self.les = {k: [c - k * n for c in sorted(need) if k * n <= c < (k + 1) * n] for k in (-2, -1, 1, 2)}
        assert not [c for c in need if not -2 * n <= c < 3 * n]
        self.wide = 2 * reach
        assert self.wide <= n and self.l2_hi <= 2 * n and self.l2_lo >= -n
        self.ape = {-1: list(range(n - self.wide, n)), 1: list(range(self.wide))}
        self.size = {}
        for k in (-2, -1, 1, 2):
            tiles = 3 * len(self.les[k]) + (2 if abs(k) == 1 else 0) + 1
            if abs(k) == 1:
                tiles = max(tiles, 4 * self.wide)
            self.size[k] = tiles
        self.depth = -(-self.wide // rows)
        if gy_size == 1:
            self.steps, self.slots = [], 1
        elif gy_size == 2:
            self.steps, self.slots = [None], 2
        else:
            self.steps = [d for d in range(-self.depth, self.depth + 1) if d]
            self.slots = 2 * self.depth + 1
        self.height = (self.slots + 2) * rows

    def reached(self, block):
        within = block % self.nb
        low = 1 - self.nb if within < self.nb - 1 else 0
        high = self.nb - 1 if within > 0 else -1
        return range(block + low, block + high + 2)

    def own_slot(self):
        if self.gy == 1:
            return 0
        return lax.axis_index("gy") if self.gy == 2 else self.depth

    def slot_of(self, step):
        return 1 - lax.axis_index("gy") if step is None else self.depth + step

    def near(self):
        return [s for s in self.steps if s is None or abs(s) == 1]

    def inside(self, step):
        if step is None:
            return None
        row = lax.axis_index("gy") + step
        return jnp.where((row >= 0) & (row < self.gy), 1.0, 0.0).astype(jnp.float32)

    def row(self, slot):
        return self.rows + self.rows * slot


def runs(values):
    out = []
    for pos, v in enumerate(values):
        if out and out[-1][0] + out[-1][2] == v:
            out[-1][2] += 1
        else:
            out.append([v, pos, 1])
    return out


def roll_z(tile, j):
    width = tile.shape[-1]
    return pltpu.roll(tile, (-j) % width, tile.ndim - 1)


def pack_kernel(plan, off_ref, wgt_ref, x_ref, *outs):
    n, nb = plan.n, plan.nb
    out_of = dict(zip((-2, -1, 1, 2), outs))
    is_les = lax.axis_index("grp") == 0

    @pl.when(is_les)
    def _():
        rowid = lax.broadcasted_iota(jnp.int32, x_ref.shape[-2:], 0)
        info = jnp.zeros(x_ref.shape[-2:], jnp.float32)
        for k in range(nb):
            info = jnp.where(rowid == k, off_ref[k].astype(jnp.float32), info)
            info = jnp.where(rowid == nb + k, wgt_ref[k], info)
        for k, out in out_of.items():
            cells = plan.les[k]
            for c in range(3):
                for first, pos, length in runs(cells):
                    at = c * len(cells) + pos
                    out[at : at + length] = x_ref[0, c, first : first + length]
            at = 3 * len(cells)
            if abs(k) == 1:
                first = n - 2 if k < 0 else 0
                out[at : at + 2] = x_ref[0, 3, first : first + 2]
                at += 2
            out[at] = info

    @pl.when(jnp.logical_not(is_les))
    def _():
        for k, out in out_of.items():
            if abs(k) == 1:
                first = plan.ape[k][0]
                for c in range(4):
                    out[c * plan.wide : (c + 1) * plan.wide] = x_ref[0, c, first : first + plan.wide]
            else:
                out[...] = jnp.zeros_like(out)


def load(ref, c, cell, row, rows=8):
    return ref[c, cell, pl.ds(row, rows), :]


def les_point(ref, cell, row, comps, spread_of):
    own = [load(ref, c, cell, row) for c in range(comps)]
    xp = [load(ref, c, cell + 1, row) for c in range(comps)]
    xm = [load(ref, c, cell - 1, row) for c in range(comps)]
    yp = [load(ref, c, cell, row + 1) for c in range(comps)]
    ym = [load(ref, c, cell, row - 1) for c in range(comps)]
    zp = [roll_z(f, 1) for f in own]
    zm = [roll_z(f, -1) for f in own]
    vort_x = (yp[2] - ym[2]) - (zp[1] - zm[1])
    vort_y = (zp[0] - zm[0]) - (xp[2] - xm[2])
    vort_z = (xp[1] - xm[1]) - (yp[0] - ym[0])
    lamb = [
        0.5 * (vort_y * own[2] - vort_z * own[1]),
        0.5 * (vort_z * own[0] - vort_x * own[2]),
        0.5 * (vort_x * own[1] - vort_y * own[0]),
    ]
    spread = [
        ((xp[c] + xm[c]) + (yp[c] + ym[c])) + (zp[c] + zm[c]) - 6.0 * own[c] for c in spread_of
    ]
    tend = [viscosity * s for s in spread]
    if comps == 4 and len(tend) == 4:
        moved = (
            own[0] * (xp[3] - xm[3]) + own[1] * (yp[3] - ym[3]) + own[2] * (zp[3] - zm[3])
        )
        tend[3] = tend[3] - 0.5 * moved
    for c in range(min(3, len(tend))):
        tend[c] = tend[c] - lamb[c]
    return own, lamb, tend


def gather_les(plan, dst, comps, x, near, messages, base, cells_lo, cells_hi):
    row = base
    for c in range(comps):
        dst[c, -cells_lo : plan.n - cells_lo, pl.ds(row, plan.rows), :] = x[c]
        for k, ref in messages.items():
            cells = plan.les[k]
            if c < 3:
                for first, pos, length in runs(cells):
                    lo = max(first + k * plan.n, cells_lo)
                    hi = min(first + length + k * plan.n, cells_hi)
                    if lo >= hi:
                        continue
                    at = c * len(cells) + pos + lo - (first + k * plan.n)
                    dst[c, lo - cells_lo : hi - cells_lo, pl.ds(row, plan.rows), :] = ref[at : at + hi - lo]
            elif abs(k) == 1:
                at = 3 * len(cells)
                lo = -2 if k < 0 else plan.n
                dst[c, lo - cells_lo : lo + 2 - cells_lo, pl.ds(row, plan.rows), :] = ref[at : at + 2]


def source_kernel(plan, off_ref, wgt_ref, *refs):
    msgs = 5
    tiles = [refs[i * msgs : (i + 1) * msgs] for i in range(1 + len(plan.steps))]
    out_ref = refs[msgs * len(tiles)]
    field, pred, lamb1, lamb2, side, summed, summed_y, ape, ape_d = refs[msgs * len(tiles) + 1 :]
    is_les = lax.axis_index("grp") == 0
    keys = (-2, -1, 1, 2)

    @pl.when(is_les)
    def _():
        les_source(plan, off_ref, wgt_ref, tiles, keys, out_ref, field, pred, lamb1, lamb2, side, summed, summed_y)

    @pl.when(jnp.logical_not(is_les))
    def _():
        ape_base(plan, tiles, keys, out_ref, ape, ape_d)


def pads(plan):
    return (0, (plan.slots + 1) * plan.rows)


def open_pad(plan):
    if plan.gy == 2:
        return [plan.own_slot() * (plan.slots + 1) * plan.rows]
    return list(pads(plan)) if plan.slots == 1 else []


def les_source(plan, off_ref, wgt_ref, tiles, keys, out_ref, field, pred, lamb1, lamb2, side, summed, summed_y):
    n, nb, bc, rows = plan.n, plan.nb, plan.bc, plan.rows
    own = plan.row(plan.own_slot())
    zero_cells = jnp.zeros((field.shape[1], rows, field.shape[3]), jnp.float32)
    for c in range(3):
        for pad in pads(plan):
            field[c, :, pl.ds(pad, rows), :] = zero_cells
        for pad in open_pad(plan):
            pred[c, :, pl.ds(pad, rows), :] = zero_cells[: pred.shape[1]]
    gather_les(plan, field, 3, tiles[0][0][0], False, dict(zip(keys, tiles[0][1:])), own, plan.f_lo, plan.f_hi)
    for step, tile in zip(plan.steps, tiles[1:]):
        gather_les(plan, field, 3, tile[0][0], True, dict(zip(keys, tile[1:])), plan.row(plan.slot_of(step)), plan.f_lo, plan.f_hi)

    def first(i, carry):
        cell = i + plan.pr_lo - plan.f_lo
        here, lamb, tend = les_point(field, cell, own, 3, (0, 1, 2))
        for c in range(3):
            lamb1[c, cell] = lamb[c]
            pred[c, i, pl.ds(own, rows), :] = here[c] + les_time_step * tend[c]
        for k, step in enumerate(plan.near()):
            row = plan.row(plan.slot_of(step))
            inside = plan.inside(step)
            here, lamb, tend = les_point(field, cell, row, 3, (0, 1, 2))
            moved = [here[c] + les_time_step * tend[c] for c in range(3)]
            if inside is not None:
                lamb[1] = lamb[1] * inside
                moved = [m * inside for m in moved]
            side[k, cell] = lamb[1]
            for c in range(3):
                pred[c, i, pl.ds(row, rows), :] = moved[c]
        return carry

    lax.fori_loop(0, plan.pr_hi - plan.pr_lo, first, 0)

    for lo, _, length in runs([b * bc + k - plan.f_lo for b in plan.extra for k in range(bc)]):

        def more(i, carry, lo=lo):
            _, lamb, _ = les_point(field, lo + i, own, 3, ())
            for c in range(3):
                lamb1[c, lo + i] = lamb[c]
            return carry

        lax.fori_loop(0, length, more, 0, unroll=2)

    def second(i, carry):
        _, lamb, _ = les_point(pred, i + plan.l2_lo - plan.pr_lo, own, 3, ())
        for c in range(3):
            lamb2[c, i + plan.l2_lo - plan.f_lo] = lamb[c]
        return carry

    lax.fori_loop(0, plan.l2_hi - plan.l2_lo, second, 0, unroll=2)

    shape = (rows, field.shape[3])
    info = {k: ref for k, ref in zip(keys, tiles[0][1:])}

    def maps(b):
        k = b // nb
        i = b % nb
        if k == 0:
            return (
                jnp.full(shape, off_ref[i].astype(jnp.float32), jnp.float32),
                jnp.full(shape, wgt_ref[i], jnp.float32),
            )
        at = 3 * len(plan.les[k]) + (2 if abs(k) == 1 else 0)
        return (
            jnp.broadcast_to(info[k][at, i : i + 1, :], shape),
            jnp.broadcast_to(info[k][at, nb + i : nb + i + 1, :], shape),
        )

    near = plan.near()
    pad_tile = jnp.zeros((n, rows, field.shape[3]), jnp.float32)
    for pad in open_pad(plan):
        summed_y[:, pl.ds(pad, rows), :] = pad_tile
    for t in range(plan.t_lo, plan.t_hi + 1):
        shares = []
        for b in plan.src[t]:
            off, wgt = maps(b)
            shares.append((b, jnp.where(off == t - b, wgt, jnp.where(off == t - b - 1, 1.0 - wgt, 0.0))))
        first_cell = max(t * bc, -reach)
        last_cell = min((t + 1) * bc, n + reach)
        inner = 0 <= t < nb

        def total(ref, c, k):
            acc = None
            for b, share in shares:
                term = share * ref[c, b * bc - plan.f_lo + k]
                acc = term if acc is None else acc + term
            return acc

        def step_k(k, carry, t=t, inner=inner, total=total):
            for c in range(3):
                s1 = total(lamb1, c, k)
                summed[c, t * bc + k + reach] = s1
                if inner:
                    out_ref[0, c + 1, t * bc + k] = s1 + total(lamb2, c, k)
                    if c == 1:
                        summed_y[t * bc + k, pl.ds(own, rows), :] = s1
            if inner:
                for q, step in enumerate(near):
                    summed_y[t * bc + k, pl.ds(plan.row(plan.slot_of(step)), rows), :] = total(side, q, k)
            return carry

        lax.fori_loop(first_cell - t * bc, last_cell - t * bc, step_k, 0)

    half_two = 0.5 * ape_time_step * ape_time_step

    def finish(i, carry):
        grads = []
        for c in range(3):
            acc = None
            for j, wt in enumerate(drp_weights, start=1):
                term = wt * (summed[c, i + reach + j] - summed[c, i + reach - j])
                acc = term if acc is None else acc + term
            grads.append(acc)
        div = grads[0]
        for j, wt in enumerate(drp_weights, start=1):
            div = div + wt * (summed_y[i, pl.ds(own + j, rows), :] - summed_y[i, pl.ds(own - j, rows), :])
        mid = summed[2, i + reach]
        for j, wt in enumerate(drp_weights, start=1):
            div = div + wt * (roll_z(mid, j) - roll_z(mid, -j))
        out_ref[0, 0, i] = half_two * div
        for c in range(3):
            out_ref[0, c + 1, i] = (half_two * mean_flow) * grads[c] - (0.5 * ape_time_step) * out_ref[0, c + 1, i]
        return carry

    lax.fori_loop(0, n, finish, 0)


def ape_point(ref, cell, row, comps):
    def along_x(c):
        acc = None
        for j, wt in enumerate(drp_weights, start=1):
            term = wt * (load(ref, c, cell + j, row) - load(ref, c, cell - j, row))
            acc = term if acc is None else acc + term
        return acc

    def along_y(c):
        acc = None
        for j, wt in enumerate(drp_weights, start=1):
            term = wt * (load(ref, c, cell, row + j) - load(ref, c, cell, row - j))
            acc = term if acc is None else acc + term
        return acc

    def along_z(c):
        mid = load(ref, c, cell, row)
        acc = None
        for j, wt in enumerate(drp_weights, start=1):
            term = wt * (roll_z(mid, j) - roll_z(mid, -j))
            acc = term if acc is None else acc + term
        return acc

    xs = {0: along_x(0), 1: along_x(1)}
    out = {0: -mean_flow * xs[0] - (xs[1] + along_y(2) + along_z(3))}
    if 1 in comps:
        out[1] = -mean_flow * xs[1] - xs[0]
    if 2 in comps:
        out[2] = -mean_flow * along_x(2) - along_y(0)
    if 3 in comps:
        out[3] = -mean_flow * along_x(3) - along_z(0)
    return out


def ape_base(plan, tiles, keys, out_ref, ape, ape_d):
    n, rows, wide = plan.n, plan.rows, plan.wide
    own = plan.row(plan.own_slot())
    blank = jnp.zeros((ape.shape[1], rows, ape.shape[3]), jnp.float32)
    for c in (0, 2):
        for pad in pads(plan):
            ape[c, wide : wide + n, pl.ds(pad, rows), :] = blank[:n]
        for pad in open_pad(plan):
            ape_d[c, reach : reach + n, pl.ds(pad, rows), :] = blank[:n]
    for c in (0, 2):
        for pad in open_pad(plan):
            ape[c, reach:wide, pl.ds(pad, rows), :] = blank[: wide - reach]
            ape[c, wide + n : wide + n + reach, pl.ds(pad, rows), :] = blank[:reach]
    for step, tile in zip([0] + plan.steps, tiles):
        main = tile is tiles[0]
        row = own if main else plan.row(plan.slot_of(step))
        msg = dict(zip(keys, tile[1:]))
        cut = wide if main else reach
        for c in range(4):
            ape[c, wide : wide + n, pl.ds(row, rows), :] = tile[0][0, c]
            left, right = msg[-1], msg[1]
            ape[c, wide - cut : wide, pl.ds(row, rows), :] = left[(c + 1) * wide - cut : (c + 1) * wide]
            ape[c, wide + n : wide + n + cut, pl.ds(row, rows), :] = right[c * wide : c * wide + cut]

    def first(i, carry):
        got = ape_point(ape, i + reach, own, (0, 1, 2, 3))
        for c in range(4):
            ape_d[c, i, pl.ds(own, rows), :] = got[c]
        return carry

    lax.fori_loop(0, n + 2 * reach, first, 0)

    for step in plan.near():
        row = plan.row(plan.slot_of(step))
        inside = plan.inside(step)

        def beside(i, carry, row=row, inside=inside):
            got = ape_point(ape, i + wide, row, (0, 2))
            for c in (0, 2):
                ape_d[c, i + reach, pl.ds(row, rows), :] = got[c] if inside is None else got[c] * inside
            return carry

        lax.fori_loop(0, n, beside, 0)

    half_two = 0.5 * ape_time_step * ape_time_step

    def second(i, carry):
        got = ape_point(ape_d, i + reach, own, (0, 1, 2, 3))
        for c in range(4):
            here = load(ape, c, i + wide, own)
            rate = load(ape_d, c, i + reach, own)
            out_ref[0, c, i] = here + ape_time_step * rate + half_two * got[c]
        return carry

    lax.fori_loop(0, n, second, 0)


def les_kernel(plan, *refs):
    msgs = 3
    tiles = [refs[i * msgs : (i + 1) * msgs] for i in range(1 + len(plan.steps))]
    out_ref, field, pred = refs[msgs * len(tiles) :]

    @pl.when(lax.axis_index("grp") == 0)
    def _():
        n, rows = plan.n, plan.rows
        own = plan.row(plan.own_slot())
        blank = jnp.zeros((n + 4, rows, field.shape[3]), jnp.float32)
        for c in range(4):
            for pad in pads(plan):
                field[c, :, pl.ds(pad, rows), :] = blank
            for pad in open_pad(plan):
                pred[c, :, pl.ds(pad, rows), :] = blank[: n + 2]
        gather_les(plan, field, 4, tiles[0][0][0], False, dict(zip((-1, 1), tiles[0][1:])), own, -2, n + 2)
        for step, tile in zip(plan.steps, tiles[1:]):
            gather_les(plan, field, 4, tile[0][0], True, dict(zip((-1, 1), tile[1:])), plan.row(plan.slot_of(step)), -2, n + 2)

        def first(i, carry):
            here, _, tend = les_point(field, i + 1, own, 4, (0, 1, 2, 3))
            for c in range(4):
                pred[c, i, pl.ds(own, rows), :] = here[c] + les_time_step * tend[c]
            for step in plan.near():
                row = plan.row(plan.slot_of(step))
                inside = plan.inside(step)
                here, _, tend = les_point(field, i + 1, row, 4, (0, 1, 2, 3))
                for c in range(4):
                    moved = here[c] + les_time_step * tend[c]
                    pred[c, i, pl.ds(row, rows), :] = moved if inside is None else moved * inside
            return carry

        lax.fori_loop(0, n + 2, first, 0)

        def second(i, carry):
            here, _, tend = les_point(pred, i + 1, own, 4, (0, 1, 2, 3))
            for c in range(4):
                start = load(field, c, i + 2, own)
                out_ref[0, c, i] = 0.5 * (start + (here[c] + les_time_step * tend[c]))
            return carry

        lax.fori_loop(0, n, second, 0)


def smem():
    return pl.BlockSpec(memory_space=pltpu.SMEM)


def vmem():
    return pl.BlockSpec(memory_space=pltpu.VMEM)


def on_device(flow_state, block_offset, block_weight):
    comps, n, rows, nz = flow_state.shape[1:]
    groups, ring, walls = [lax.axis_size(a) for a in ("grp", "gx", "gy")]
    plan = Plan(n, block_offset.shape[0], rows, walls)
    f32 = jnp.float32
    keys = (-2, -1, 1, 2)
    packed = pl.pallas_call(
        lambda *r: pack_kernel(plan, *r),
        name="pack",
        compiler_params=pltpu.CompilerParams(vmem_limit_bytes=8 * 2**20),
        in_specs=[smem(), smem(), vmem()],
        out_specs=[vmem()] * 4,
        out_shape=[jax.ShapeDtypeStruct((plan.size[k], rows, nz), f32) for k in keys],
    )(block_offset, block_weight, flow_state)

    def along(block, shift):
        return lax.ppermute(block, "gx", [((i + shift) % ring, i) for i in range(ring)])

    def beside(block, step):
        if step is None:
            return lax.ppermute(block, "gy", [(0, 1), (1, 0)])
        return lax.ppermute(block, "gy", [(i + step, i) for i in range(walls) if 0 <= i + step < walls])

    got = [along(p, k) for k, p in zip(keys, packed)]
    tiles = [[flow_state] + got]
    for step in plan.steps:
        tiles.append([beside(flow_state, step)] + [beside(g, step) for g in got])

    def scratch(*shape):
        return pltpu.VMEM(shape, f32)

    cells = plan.f_hi - plan.f_lo
    h = plan.height
    part = pl.pallas_call(
        lambda *r: source_kernel(plan, *r),
        name="source",
        compiler_params=pltpu.CompilerParams(vmem_limit_bytes=24 * 2**20),
        in_specs=[smem(), smem()] + [vmem()] * (5 * len(tiles)),
        out_specs=vmem(),
        out_shape=jax.ShapeDtypeStruct(flow_state.shape, f32),
        scratch_shapes=[
            scratch(3, cells, h, nz),
            scratch(3, plan.pr_hi - plan.pr_lo, h, nz),
            scratch(3, cells, rows, nz),
            scratch(3, cells, rows, nz),
            scratch(max(1, len(plan.near())), cells, rows, nz),
            scratch(3, n + 2 * reach, rows, nz),
            scratch(n, h, nz),
            scratch(4, n + 2 * plan.wide, h, nz),
            scratch(4, n + 2 * reach, h, nz),
        ],
    )(block_offset, block_weight, *[a for t in tiles for a in t])
    handed = lax.ppermute(part, "grp", [(i, (i + 1) % groups) for i in range(groups)])
    les = pl.pallas_call(
        lambda *r: les_kernel(plan, *r),
        name="les",
        compiler_params=pltpu.CompilerParams(vmem_limit_bytes=16 * 2**20),
        in_specs=[vmem()] * (3 * len(tiles)),
        out_specs=vmem(),
        out_shape=jax.ShapeDtypeStruct(flow_state.shape, f32),
        scratch_shapes=[scratch(4, n + 4, h, nz), scratch(4, n + 2, h, nz)],
    )(*[a for t in tiles for a in (t[0], t[2], t[3])])
    return jnp.where(lax.axis_index("grp") == 0, les, part + handed)


def solution(mesh):
    placed = (P("grp", None, "gx", "gy", None), P("gx"), P("gx"))
    return jax.shard_map(
        on_device,
        mesh=mesh,
        in_specs=placed,
        out_specs=P("grp", None, "gx", "gy", None),
        check_vma=False,
    )
```
